8 devices in a mesh: data: 8 (over z, y, x, core).
Axes of the slice: x: 2, y: 2, z: 1, core: 2. Of those that a mesh axis runs over, the one named last changes fastest.
Arguments:
- tokens: bfloat16 [16384, 1280], P('data')
- targets: bfloat16 [16384, 1280], P('data')
- w_in: bfloat16 [4, 1280, 5120], replicated
- w_out: bfloat16 [4, 5120, 1280], replicated
Outputs:
- output 1: float32 [4, 1280, 5120], replicated
- output 2: float32 [4, 5120, 1280], replicated
All inputs are finite; a program needn't handle non-finite values.
Results may differ from the reference program's by a relative error of at most 0.0072231.
Values are sent between devices in bfloat16 or wider.
A program may use at most 1.25 GiB of HBM per device.

```python
import math
import jax
import jax.numpy as jnp
from jax import lax

D = 1280
FF = 5120
LAYERS = 4
TOK_DEV = 2048
GROUP = 8


def setup_inputs(seed: int = 0) -> dict:
    rng_keys = jax.random.split(jax.random.key(seed), 4)
    num_tokens = GROUP * TOK_DEV
    tok_f32 = jax.random.normal(rng_keys[0], (num_tokens, D), jnp.float32)
    tgt_f32 = tok_f32 + 2.0 * jax.random.normal(rng_keys[1], (num_tokens, D), jnp.float32)
    w_in = jax.random.normal(rng_keys[2], (LAYERS, D, FF), jnp.float32) * D ** -0.5
    w_raw = jax.random.normal(rng_keys[3], (LAYERS, FF, D), jnp.float32)
    w_out = (w_raw - jnp.mean(w_raw, axis=1, keepdims=True)) * FF ** -0.5
    return {
        "tokens": tok_f32.astype(jnp.bfloat16),
        "targets": tgt_f32.astype(jnp.bfloat16),
        "w_in": w_in.astype(jnp.bfloat16),
        "w_out": w_out.astype(jnp.bfloat16),
    }


def gelu_fn(value):
    return jax.nn.gelu(value, approximate=True)


def micro_grads(tok_mb, tgt_mb, w_in, w_out, scale):
    def fwd_step(hidden, weights):
        pre_act = jnp.dot(hidden, weights[0], preferred_element_type=jnp.float32).astype(jnp.bfloat16)
        gelu_out = gelu_fn(pre_act.astype(jnp.float32)).astype(jnp.bfloat16)
        branch = jnp.dot(gelu_out, weights[1], preferred_element_type=jnp.float32)
        next_hidden = (hidden.astype(jnp.float32) + branch).astype(jnp.bfloat16)
        return next_hidden, (hidden, pre_act, gelu_out)

    last_hidden, saved = lax.scan(fwd_step, tok_mb, (w_in, w_out))
    cotangent = ((last_hidden.astype(jnp.float32) - tgt_mb.astype(jnp.float32)) * scale).astype(jnp.bfloat16)

    def bwd_step(cot_in, layer_data):
        layer_in, pre_act, gelu_out, win_layer, wout_layer = layer_data
        g_out = jnp.dot(gelu_out.T, cot_in, preferred_element_type=jnp.float32)
        d_act = jnp.dot(cot_in, wout_layer.T, preferred_element_type=jnp.float32)
        _, gelu_vjp = jax.vjp(gelu_fn, pre_act.astype(jnp.float32))
        d_pre = gelu_vjp(d_act)[0].astype(jnp.bfloat16)
        g_in = jnp.dot(layer_in.T, d_pre, preferred_element_type=jnp.float32)
        back_prod = jnp.dot(d_pre, win_layer.T, preferred_element_type=jnp.float32)
        next_cot = (cot_in.astype(jnp.float32) + back_prod).astype(jnp.bfloat16)
        return next_cot, (g_in, g_out)

    _, grads = lax.scan(bwd_step, cotangent, (saved[0], saved[1], saved[2], w_in, w_out), reverse=True)
    return grads


def reference(tokens, targets, w_in, w_out):
    num_tokens = tokens.shape[0]
    scale = 1.0 / math.sqrt(num_tokens)
    half_rows = TOK_DEV // 2
    tok_mbs = tokens.reshape(2 * GROUP, half_rows, D)
    tgt_mbs = targets.reshape(2 * GROUP, half_rows, D)

    def accumulate(carry, batch):
        g_in, g_out = micro_grads(batch[0], batch[1], w_in, w_out, scale)
        return (carry[0] + g_in, carry[1] + g_out), None

    zero_grads = (jnp.zeros((LAYERS, D, FF), jnp.float32), jnp.zeros((LAYERS, FF, D), jnp.float32))
    totals, _ = lax.scan(accumulate, zero_grads, (tok_mbs, tgt_mbs))
    return totals[0], totals[1]
```

```python
import math
import jax
import jax.numpy as jnp
from jax import lax
from jax.experimental import pallas as pl
from jax.sharding import PartitionSpec as P


NN = (((1,), (0,)), ((), ()))
NT = (((1,), (1,)), ((), ()))
TN = (((0,), (0,)), ((), ()))
F32 = jnp.float32
BF16 = jnp.bfloat16
ROOT = math.sqrt(2.0 / math.pi)
CUBIC = 0.044715

LAYERS = 4
SENDS = "XYDEG"
PLACES = {"F": ("F", 0), "Q": ("X", 2), "R": ("E", 1), "T": ("G", 3)}
PIECES = {f"{kind}{layer}": 2 for layer in range(LAYERS) for kind in "AB"} | {"B0": 4}
COST = {"u": 39.7, "d": 33.7, "v": 40.7, "g": 33.7, "grad": 11.8, "sum": 8.5, "place": 5.0, "split": 4.0,
        "act": 112.0, "link": 140.0, "core": 13.0, "wake": 2.0, "ahead": 100.0}


def issue_order(pieces, cost):
    plan = [("X", "h0")]
    for layer in range(LAYERS):
        plan += [("o", "u", layer), ("o", "d", layer)]
        if layer + 1 in (1, 3):
            plan.append(("X", f"h{layer + 1}"))
    plan.append(("X", f"g{LAYERS}"))
    plan += [("f", "u", 0), ("f", "u", 1), ("f", "d", 1), ("f", "u", 2), ("f", "u", 3)]
    for layer in reversed(range(LAYERS)):
        for kind in "AB":
            name = f"{kind}{layer}"
            if kind == "B":
                plan += [("o", "v", layer), ("f", "v", layer)]
            plan += [(name, "s", "o"), (name, "s", "f"), ("D", name), (name, "m", "o"), (name, "m", "f")]
            if pieces[name] > 1:
                plan.append(("S", name))
            plan += [("Y", name, piece) for piece in range(pieces[name])]
        if layer:
            plan += [("o", "g", layer), ("f", "g", layer)]
    needs = {("f", "u", 0): ("X", "h0"), ("f", "u", 1): ("X", "h1"), ("f", "u", 3): ("X", "h3"), (f"A{LAYERS - 1}", "s", "f"): ("X", f"g{LAYERS}")}
    for name in pieces:
        needs[name, "m", "f"] = ("D", name)
    order, landed, free = [], {}, {"X": 0.0, "Y": 0.0}
    clock = 0.0
    summing, passing, placing = [], [], []

    def run(item):
        nonlocal clock
        clock = max(clock, landed.get(needs.get(item), 0.0))
        mark = item[0]
        if mark in PLACES:
            clock += cost["sum" if mark == "F" else "place"] / pieces[item[1]]
        elif mark == "S":
            clock += cost["split"]
        elif mark in pieces:
            clock += cost["grad"]
        else:
            clock += cost[item[1]]
        order.append(item)

    def start(item):
        mark = item[0]
        share = 1 if len(item) == 2 else pieces[item[1]]
        if mark in free:
            length = cost["act"] if item[1] not in pieces else cost["link"] / share
            free[mark] = max(clock, free[mark]) + length
            landed[item] = free[mark] + cost["wake"]
        else:
            landed[item] = clock + cost["core"] / share + cost["wake"]
        order.append(item)
        if mark == "Y":
            summing.append(item[1:])

    def serve():
        busy = False
        for tag in [t for t in summing if landed[("Y", *t)] <= clock]:
            summing.remove(tag)
            run(("F", *tag))
            start(("X", *tag))
            start(("E", *tag))
            passing.append(tag)
            placing.append((("R", *tag), ("E", *tag)))
            busy = True
        for tag in [t for t in passing if landed[("X", *t)] <= clock]:
            passing.remove(tag)
            start(("G", *tag))
            placing.extend([(("Q", *tag), ("X", *tag)), (("T", *tag), ("G", *tag))])
            busy = True
        return busy

    def put():
        for entry in placing:
            if landed[entry[1]] <= clock:
                placing.remove(entry)
                run(entry[0])
                return True
        return False

    for item in plan:
        if item[0] in SENDS:
            start(item)
            continue
        serve()
        while free["Y"] - clock > cost["ahead"] and put():
            serve()
        run(item)
    while summing or passing or placing:
        if not (serve() or put()):
            times = [landed[("Y", *t)] for t in summing] + [landed[("X", *t)] for t in passing] + [landed[e[1]] for e in placing]
            clock = max(clock, min(times))
    return order


def gelu_fn(value):
    return jax.nn.gelu(value, approximate=True)


def gelu_slope(value):
    square = value * value
    t = jnp.tanh(ROOT * value * (1.0 + CUBIC * square))
    plus = 0.5 + 0.5 * t
    return plus + value * plus * (1.0 - t) * (ROOT + 3.0 * ROOT * CUBIC * square)


def dot(left, right, dims):
    return lax.dot_general(left, right, dims, preferred_element_type=F32)


def blank(shape):
    return pl.pallas_call(
        lambda out: None,
        out_shape=jax.ShapeDtypeStruct(shape, F32),
        out_specs=pl.BlockSpec(memory_space=pl.ANY),
    )()


def solution(mesh):
    order = issue_order(PIECES, COST)
    group = mesh.shape["data"]
    to_core = [(i, i ^ 1) for i in range(group)]
    to_x = [(i, i ^ 2) for i in range(group)]
    to_y = [(i, i ^ 4) for i in range(group)]
    route = {"X": to_x, "Y": to_y, "D": to_core, "E": to_core, "G": to_core}

    def local_step(tokens, targets, w_in, w_out):
        rows = tokens.shape[0]
        layers, width, ff = w_in.shape
        blk = ff // 4
        scale = 1.0 / math.sqrt(rows * group)
        me = lax.axis_index("data") & 3
        starts = [pl.multiple_of((me ^ flip) * blk, blk) for flip in range(4)]
        grads = {"A": blank((layers, ff, width)), "B": blank((layers, width, ff))}
        val = {("o", "h0"): tokens}

        def up(side, layer):
            pre = dot(val[side, f"h{layer}"], w_in[layer], NN).astype(BF16)
            act = gelu_fn(pre.astype(F32)).astype(BF16)
            val[side, f"u{layer}"], val[side, f"a{layer}"] = lax.optimization_barrier((pre, act))

        def down(side, layer):
            hidden = val[side, f"h{layer}"].astype(F32) + dot(val[side, f"a{layer}"], w_out[layer], NN)
            hidden = hidden.astype(BF16)
            if layer < layers - 1:
                val[side, f"h{layer + 1}"] = hidden
            else:
                val[side, f"g{layers}"] = ((hidden.astype(F32) - targets.astype(F32)) * scale).astype(BF16)

        def back_act(side, layer):
            cot, pre = lax.optimization_barrier((val[side, f"g{layer + 1}"], val[side, f"u{layer}"]))
            d_act = dot(cot, w_out[layer], NT)
            d_pre = (d_act * gelu_slope(pre.astype(F32))).astype(BF16)
            val[side, f"v{layer}"] = lax.optimization_barrier(d_pre)

        def back_hidden(side, layer):
            total = val[side, f"g{layer + 1}"].astype(F32) + dot(val[side, f"v{layer}"], w_in[layer], NT)
            val[side, f"g{layer}"] = total.astype(BF16)

        def partial_sum(name, block, side):
            kind, layer = name[0], int(name[1])
            start = starts[1] if block == "s" else starts[0]
            if kind == "A":
                left, right = val[side, f"a{layer}"], val[side, f"g{layer + 1}"]
                left = lax.dynamic_slice_in_dim(left, start, blk, axis=1)
            else:
                left, right = val[side, f"h{layer}"], val[side, f"v{layer}"]
                right = lax.dynamic_slice_in_dim(right, start, blk, axis=1)
            total = dot(left, right, TN)
            if side == "f":
                total = total + val[name, block]
                if block == "m":
                    total = total + val["D", name]
            else:
                total = lax.optimization_barrier(total)
            val[name, block] = val[name, 0] = total

        def split(name):
            own = val[name, "m"]
            step = own.shape[0] // PIECES[name]
            for piece in range(PIECES[name]):
                val[name, piece] = own[piece * step:(piece + 1) * step]

        def place(mark, name, piece):
            if mark == "F":
                val["F", name, piece] = val[name, piece] + val["Y", name, piece]
            source, which = PLACES[mark]
            block, start = val[source, name, piece], starts[which]
            kind, layer = name[0], int(name[1])
            first = piece * block.shape[0]
            where = (layer, start + first, 0) if kind == "A" else (layer, first, start)
            grads[kind] = lax.dynamic_update_slice(grads[kind], block[None], where)

        def operation(item):
            mark = item[0]
            if mark in PIECES:
                partial_sum(*item)
            elif mark == "S":
                split(item[1])
            elif mark in PLACES:
                place(*item)
            else:
                {"u": up, "d": down, "v": back_act, "g": back_hidden}[item[1]](mark, item[2])

        def transfer(item):
            mark, rest = item[0], item[1:]
            if rest[0] not in PIECES:
                val["f", rest[0]] = lax.ppermute(val["o", rest[0]], "data", to_x)
                return
            source = {"X": ("F", *rest), "E": ("F", *rest), "G": ("X", *rest), "Y": rest, "D": (rest[0], "s")}[mark]
            val[item] = lax.ppermute(val[source], "data", route[mark])

        for item in order:
            (transfer if item[0] in SENDS else operation)(item)
        return grads["B"], grads["A"]

    return jax.shard_map(local_step, mesh=mesh, in_specs=(P("data"), P("data"), P(), P()), out_specs=(P(), P()), check_vma=False)
```

```python
import math
import jax
import jax.numpy as jnp
from jax import lax
from jax.experimental import pallas as pl
from jax.experimental.pallas import tpu as pltpu
from jax.sharding import PartitionSpec as P


NN = (((1,), (0,)), ((), ()))
NT = (((1,), (1,)), ((), ()))
TN = (((0,), (0,)), ((), ()))
F32 = jnp.float32
BF16 = jnp.bfloat16
ROOT = math.sqrt(2.0 / math.pi)
CUBIC = 0.044715

LAYERS = 4
SENDS = "XYDEG"
PLACES = {"F": ("F", 0), "Q": ("X", 2), "R": ("E", 1), "T": ("G", 3)}
PIECES = {f"{kind}{layer}": 2 for layer in range(LAYERS) for kind in "AB"} | {"B0": 4}
COST = {"u": 32.0, "d": 32.0, "v": 39.0, "g": 32.0, "grad": 18.0, "sum": 11.0, "place": 7.5,
        "act": 112.0, "link": 140.0, "core": 13.0, "wake": 2.0, "ahead": 250.0}


def sums(name, pieces, after, between):
    sends = [("Y", name, piece) for piece in range(pieces[name])]
    return [(name, "s"), ("D", name), *between[:1], (name, "m"), *sends, *between[1:], *after]


def issue_order(pieces, cost):
    plan = [("X", "h0")]
    for layer in range(LAYERS):
        plan += [("o", "u", layer), ("o", "d", layer)]
        if layer == 1:
            plan.append(("X", "h2"))
    plan.append(("X", f"g{LAYERS}"))
    plan += [("f", "u", 2), ("f", "d", 2), ("f", "u", 3)]
    for layer in reversed(range(LAYERS)):
        one, two = f"A{layer}", f"B{layer}"
        fill = [("o", "v", layer), ("f", "v", layer)]
        plan += sums(one, pieces, fill if layer == LAYERS - 1 else [], fill if layer < LAYERS - 1 else [])
        fill = [("o", "g", layer), ("f", "g", layer)] if layer else []
        if layer == LAYERS - 2:
            fill += [("f", "u", 0), ("f", "d", 0), ("f", "u", 1)]
        plan += sums(two, pieces, [], fill)
    needs = {("f", "u", 2): ("X", "h2"), ("f", "u", 0): ("X", "h0"), (f"A{LAYERS - 1}", "s"): ("X", f"g{LAYERS}")}
    for name in pieces:
        needs[name, "m"] = ("D", name)
    order, landed, free = [], {}, {"X": 0.0, "Y": 0.0}
    clock = 0.0
    summing, passing, placing = [], [], []

    def run(item):
        nonlocal clock
        clock = max(clock, landed.get(needs.get(item), 0.0))
        mark = item[0]
        if mark in PLACES:
            clock += cost["sum" if mark == "F" else "place"] / pieces[item[1]]
        elif mark in pieces:
            clock += cost["grad"]
        else:
            clock += cost[item[1]]
        order.append(item)

    def start(item):
        mark = item[0]
        share = 1 if len(item) == 2 else pieces[item[1]]
        if mark in free:
            length = cost["act"] if item[1] not in pieces else cost["link"] / share
            free[mark] = max(clock, free[mark]) + length
            landed[item] = free[mark] + cost["wake"]
        else:
            landed[item] = clock + cost["core"] / share + cost["wake"]
        order.append(item)
        if mark == "Y":
            summing.append(item[1:])

    def serve():
        busy = False
        for tag in [t for t in summing if landed[("Y", *t)] <= clock]:
            summing.remove(tag)
            run(("F", *tag))
            start(("X", *tag))
            start(("E", *tag))
            passing.append(tag)
            placing.append((("R", *tag), ("E", *tag)))
            busy = True
        for tag in [t for t in passing if landed[("X", *t)] <= clock]:
            passing.remove(tag)
            start(("G", *tag))
            placing.extend([(("Q", *tag), ("X", *tag)), (("T", *tag), ("G", *tag))])
            busy = True
        return busy

    def put():
        for entry in placing:
            if landed[entry[1]] <= clock:
                placing.remove(entry)
                run(entry[0])
                return True
        return False

    for item in plan:
        if item[0] in SENDS:
            start(item)
            continue
        serve()
        while free["Y"] - clock > cost["ahead"] and put():
            serve()
        run(item)
    while summing or passing or placing:
        if not (serve() or put()):
            times = [landed[("Y", *t)] for t in summing] + [landed[("X", *t)] for t in passing] + [landed[e[1]] for e in placing]
            clock = max(clock, min(times))
    return order


def gelu_fn(value):
    return jax.nn.gelu(value, approximate=True)


def gelu_slope(value):
    square = value * value
    t = jnp.tanh(value * (ROOT + (ROOT * CUBIC) * square))
    return (0.5 + 0.5 * t) + (value * (0.5 * ROOT + (1.5 * ROOT * CUBIC) * square)) * (1.0 - t * t)


def dot(left, right, dims):
    return lax.dot_general(left, right, dims, preferred_element_type=F32)


def blank(shape):
    return pl.pallas_call(
        lambda out: None,
        out_shape=jax.ShapeDtypeStruct(shape, F32),
        out_specs=pl.BlockSpec(memory_space=pl.ANY),
    )()


PARAMS = pltpu.CompilerParams(vmem_limit_bytes=67_043_328)


def work(rows, depth, columns, moved):
    return pl.CostEstimate(flops=2 * rows * depth * columns, bytes_accessed=moved, transcendentals=0)


def up_kernel(layer, hidden, w_in):
    rows, width = hidden.shape
    ff = w_in.shape[2]
    tile, chunk = 512, 128

    def body(h_ref, w_ref, u_ref, a_ref):
        last = None
        for first in [*range(0, rows, chunk), None]:
            if first is not None:
                part = pl.ds(first, chunk)
                u_ref[part, :] = dot(h_ref[part, :], w_ref[0], NN).astype(BF16)
            if last is not None:
                part = pl.ds(last, chunk)
                a_ref[part, :] = gelu_fn(u_ref[part, :].astype(F32)).astype(BF16)
            last = first

    return pl.pallas_call(
        body,
        grid=(ff // tile,),
        in_specs=[pl.BlockSpec((rows, width), lambda j: (0, 0)), pl.BlockSpec((1, width, tile), lambda j: (layer, 0, j))],
        out_specs=[pl.BlockSpec((rows, tile), lambda j: (0, j))] * 2,
        out_shape=[jax.ShapeDtypeStruct((rows, ff), BF16)] * 2,
        compiler_params=PARAMS,
        cost_estimate=work(rows, width, ff, 60_000_000),
    )(hidden, w_in)


def down_kernel(layer, value, weights, base, dims, target=None, scale=1.0):
    rows, ff = value.shape
    width = base.shape[1]
    tile = 512
    chunk = 128 if dims == NN else 256
    steps = ff // tile
    if dims == NN:
        w_spec = pl.BlockSpec((1, tile, width), lambda j: (layer, j, 0))
    else:
        w_spec = pl.BlockSpec((1, width, tile), lambda j: (layer, 0, j))
    whole = pl.BlockSpec((rows, width), lambda j: (0, 0))

    def body(x_ref, w_ref, base_ref, *rest):
        out_ref, total = rest[-2:]
        step = pl.program_id(0)

        @pl.when(step == 0)
        def _():
            total[...] = base_ref[...].astype(F32)

        for first in range(0, rows, chunk):
            part = pl.ds(first, chunk)
            total[part, :] += dot(x_ref[part, :], w_ref[0], dims)

        @pl.when(step == steps - 1)
        def _():
            result = total[...].astype(BF16)
            if target is not None:
                result = ((result.astype(F32) - rest[0][...].astype(F32)) * scale).astype(BF16)
            out_ref[...] = result

    extra = [] if target is None else [target]
    return pl.pallas_call(
        body,
        grid=(steps,),
        in_specs=[pl.BlockSpec((rows, tile), lambda j: (0, j)), w_spec, whole] + [whole] * len(extra),
        out_specs=whole,
        out_shape=jax.ShapeDtypeStruct((rows, width), BF16),
        scratch_shapes=[pltpu.VMEM((rows, width), F32)],
        compiler_params=PARAMS,
        cost_estimate=work(rows, ff, width, 45_000_000),
    )(value, weights, base, *extra)


def back_kernel(layer, cot, w_out, pre):
    rows, width = cot.shape
    ff = pre.shape[1]
    tile, chunk = 512, 256

    def body(g_ref, w_ref, u_ref, v_ref):
        for first in range(0, rows, chunk):
            part = pl.ds(first, chunk)
            v_ref[part, :] = (dot(g_ref[part, :], w_ref[0], NT) * gelu_slope(u_ref[part, :].astype(F32))).astype(BF16)

    return pl.pallas_call(
        body,
        grid=(ff // tile,),
        in_specs=[
            pl.BlockSpec((rows, width), lambda j: (0, 0)),
            pl.BlockSpec((1, tile, width), lambda j: (layer, j, 0)),
            pl.BlockSpec((rows, tile), lambda j: (0, j)),
        ],
        out_specs=pl.BlockSpec((rows, tile), lambda j: (0, j)),
        out_shape=jax.ShapeDtypeStruct((rows, ff), BF16),
        compiler_params=PARAMS,
        cost_estimate=work(rows, width, ff, 60_000_000),
    )(cot, w_out, pre)


def gradient_kernel(which, sliced, left, right, theirs, pieces):
    rows = left[0].shape[0]
    blk = 1280
    tile, chunk = 512, 128
    height = blk // pieces
    ends = (256, 640, 896, blk)
    cuts = sorted({0, *ends, *range(0, blk, height)})
    ranges = [(first, last - first) for first, last in zip(cuts, cuts[1:])]
    half = rows // tile
    steps = 2 * half

    def spec(name, far):
        def index(k, which):
            row = jnp.maximum(k - half, 0) if far else jnp.minimum(k, half - 1)
            return row, (which[0] if name == sliced else 0)

        return pl.BlockSpec((tile, blk), index)

    def body(which_ref, lo, lf, ro, rf, *rest):
        theirs_ref = rest[0] if theirs is not None else None
        outs = rest[1 if theirs is not None else 0:][:pieces]
        total, out_sems = rest[-2 - (2 if theirs is not None else 0):][:2]
        step = pl.program_id(0)

        def product(l_ref, r_ref, first):
            return dot(l_ref[:, pl.ds(first, chunk)], r_ref[...], TN)

        if theirs is not None:
            other, other_sem = rest[-2:]
            fetch = pltpu.make_async_copy(theirs_ref, other, other_sem)

        @pl.when(step == 0)
        def _():
            if theirs is not None:
                fetch.start()
            for first in range(0, blk, chunk):
                total[pl.ds(first, chunk), :] = product(lo, ro, first)

        @pl.when(jnp.logical_and(step > 0, step < half))
        def _():
            for first in range(0, blk, chunk):
                total[pl.ds(first, chunk), :] += product(lo, ro, first)

        @pl.when(jnp.logical_and(step >= half, step < steps - 1))
        def _():
            for first in range(0, blk, chunk):
                total[pl.ds(first, chunk), :] += product(lf, rf, first)

        @pl.when(step == steps - 1)
        def _():
            if theirs is not None:
                fetch.wait()
            copies = []
            for first in range(0, blk, chunk):
                part = pl.ds(first, chunk)
                value = total[part, :] + product(lf, rf, first)
                total[part, :] = value if theirs is None else value + other[part, :]
                if first + chunk in ends:
                    for start, count in ranges[len(copies):]:
                        if start + count > first + chunk:
                            break
                        piece, offset = divmod(start, height)
                        copies.append(pltpu.make_async_copy(
                            total.at[pl.ds(start, count), :], outs[piece].at[pl.ds(offset, count), :], out_sems.at[len(copies)]))
                        copies[-1].start()
            for copy in copies:
                copy.wait()

    anywhere = pl.BlockSpec(memory_space=pl.ANY)
    extra = [] if theirs is None else [theirs]
    scratch = [pltpu.VMEM((blk, blk), F32), pltpu.SemaphoreType.DMA((len(ranges),))]
    if theirs is not None:
        scratch += [pltpu.VMEM((blk, blk), F32), pltpu.SemaphoreType.DMA(())]
    return pl.pallas_call(
        body,
        grid_spec=pltpu.PrefetchScalarGridSpec(
            num_scalar_prefetch=1,
            grid=(steps,),
            in_specs=[spec("left", False), spec("left", True), spec("right", False), spec("right", True)] + [anywhere] * len(extra),
            out_specs=[anywhere] * pieces,
            scratch_shapes=scratch,
        ),
        out_shape=[jax.ShapeDtypeStruct((blk // pieces, blk), F32)] * pieces,
        compiler_params=PARAMS,
        cost_estimate=work(2 * rows, blk, blk, 40_000_000),
    )(which, *left, *right, *extra)


def solution(mesh):
    order = issue_order(PIECES, COST)
    group = mesh.shape["data"]
    to_core = [(i, i ^ 1) for i in range(group)]
    to_x = [(i, i ^ 2) for i in range(group)]
    to_y = [(i, i ^ 4) for i in range(group)]
    route = {"X": to_x, "Y": to_y, "D": to_core, "E": to_core, "G": to_core}

    def local_step(tokens, targets, w_in, w_out):
        rows = tokens.shape[0]
        layers, width, ff = w_in.shape
        blk = ff // 4
        scale = 1.0 / math.sqrt(rows * group)
        me = lax.axis_index("data") & 3
        starts = [pl.multiple_of((me ^ flip) * blk, blk) for flip in range(4)]
        blocks = [jnp.reshape(me ^ flip, (1,)).astype(jnp.int32) for flip in range(2)]
        grads = {"A": blank((layers, ff, width)), "B": blank((layers, width, ff))}
        val = {("o", "h0"): tokens}

        def up(side, layer):
            val[side, f"u{layer}"], val[side, f"a{layer}"] = up_kernel(layer, val[side, f"h{layer}"], w_in)

        def down(side, layer):
            last = layer == layers - 1
            result = down_kernel(layer, val[side, f"a{layer}"], w_out, val[side, f"h{layer}"], NN, targets if last else None, scale)
            val[side, f"g{layers}" if last else f"h{layer + 1}"] = result

        def back_act(side, layer):
            val[side, f"v{layer}"] = back_kernel(layer, val[side, f"g{layer + 1}"], w_out, val[side, f"u{layer}"])

        def back_hidden(side, layer):
            val[side, f"g{layer}"] = down_kernel(layer, val[side, f"v{layer}"], w_in, val[side, f"g{layer + 1}"], NT)

        def partial_sum(name, block):
            kind, layer = name[0], int(name[1])
            left, right = ("a", f"g{layer + 1}") if kind == "A" else ("h", f"v{layer}")
            left = [val[side, f"{left}{layer}"] for side in "of"]
            right = [val[side, right] for side in "of"]
            mine = block == "m"
            parts = gradient_kernel(
                blocks[0 if mine else 1], "left" if kind == "A" else "right", left, right,
                val["D", name] if mine else None, PIECES[name] if mine else 1)
            if mine:
                for piece, part in enumerate(parts):
                    val[name, piece] = part
            else:
                val[name, "s"] = parts[0]

        def place(mark, name, piece):
            if mark == "F":
                val["F", name, piece] = val[name, piece] + val["Y", name, piece]
            source, which = PLACES[mark]
            block, start = val[source, name, piece], starts[which]
            kind, layer = name[0], int(name[1])
            first = piece * block.shape[0]
            where = (layer, start + first, 0) if kind == "A" else (layer, first, start)
            grads[kind] = lax.dynamic_update_slice(grads[kind], block[None], where)

        def operation(item):
            mark = item[0]
            if mark in PIECES:
                partial_sum(*item)
            elif mark in PLACES:
                place(*item)
            else:
                {"u": up, "d": down, "v": back_act, "g": back_hidden}[item[1]](mark, item[2])

        def transfer(item):
            mark, rest = item[0], item[1:]
            if rest[0] not in PIECES:
                val["f", rest[0]] = lax.ppermute(val["o", rest[0]], "data", to_x)
                return
            source = {"X": ("F", *rest), "E": ("F", *rest), "G": ("X", *rest), "Y": rest, "D": (rest[0], "s")}[mark]
            val[item] = lax.ppermute(val[source], "data", route[mark])

        for item in order:
            (transfer if item[0] in SENDS else operation)(item)
        return grads["B"], grads["A"]

    return jax.shard_map(local_step, mesh=mesh, in_specs=(P("data"), P("data"), P(), P()), out_specs=(P(), P()), check_vma=False)
```

```python
import math
import jax
import jax.numpy as jnp
from jax import lax
from jax.experimental import pallas as pl
from jax.experimental.pallas import tpu as pltpu
from jax.sharding import PartitionSpec as P


NN = (((1,), (0,)), ((), ()))
NT = (((1,), (1,)), ((), ()))
TN = (((0,), (0,)), ((), ()))
F32 = jnp.float32
BF16 = jnp.bfloat16
ROOT = math.sqrt(2.0 / math.pi)
CUBIC = 0.044715

LAYERS = 4
SENDS = "XYDEG"
PLACES = {"F": ("F", 0), "Q": ("X", 2), "R": ("E", 1), "T": ("G", 3)}
PIECES = {f"{kind}{layer}": 2 for layer in range(LAYERS) for kind in "AB"} | {"A0": 4, "B0": 8}
COST = {"w": 66.0, "g": 37.0, "u": 35.2, "b": 70.0, "v": 44.0, "grad": 19.8, "sum": 12.2, "place": 7.7, "start": 0.8,
        "act": 112.0, "link": 140.0, "core": 11.0, "wake": 1.0, "ahead": 1000.0}


def core_plan(pieces):
    def other(name):
        return [(name, "s"), ("D", name)]

    def mine(name):
        return [(name, "m"), *(("Y", name, piece) for piece in range(pieces[name]))]

    plan = [("X", "h0"), ("o", "w", 0), ("o", "w", 1), ("X", "h2"), ("o", "w", 2), ("o", "w", 3), ("X", "g4"), ("X", "h1")]
    plan += [("f", "w", 2), ("f", "u", 3), *other("A3"), *mine("A3")]
    plan += [("o", "b", 3), ("f", "b", 3), *other("B3"), *other("A2"), *mine("B3")]
    plan += [("o", "b", 2), *mine("A2"), ("f", "b", 2)]
    plan += [*other("B2"), ("f", "u", 1), *mine("B2"), *other("A1"), ("o", "b", 1), *mine("A1"), ("f", "b", 1)]
    plan += [*other("B1"), ("f", "u", 0), *mine("B1"), *other("A0"), ("o", "v", 0), *mine("A0"), ("f", "v", 0)]
    return plan + [*other("B0"), *mine("B0")]


def issue_order(pieces, cost):
    plan = core_plan(pieces)
    needs = {("f", "w", 2): ("X", "h2"), ("f", "u", 1): ("X", "h1"), ("f", "u", 0): ("X", "h0"), ("A3", "s"): ("X", "g4")}
    for name in pieces:
        needs[name, "m"] = ("D", name)
    order, landed, free = [], {}, {"X": 0.0, "Y": 0.0}
    clock = 0.0
    summing, passing, placing = [], [], []

    def run(item):
        nonlocal clock
        clock = max(clock, landed.get(needs.get(item), 0.0))
        mark = item[0]
        if mark in PLACES:
            clock += cost["sum" if mark == "F" else "place"] / pieces[item[1]]
        elif mark in pieces:
            clock += cost["grad"]
        else:
            clock += cost[item[1]]
        order.append(item)

    def start(item):
        nonlocal clock
        mark = item[0]
        clock += cost["start"]
        share = 1 if len(item) == 2 else pieces[item[1]]
        if mark in free:
            length = cost["act"] if item[1] not in pieces else cost["link"] / share
            free[mark] = max(clock, free[mark]) + length
            landed[item] = free[mark] + cost["wake"]
        else:
            landed[item] = clock + cost["core"] / share + cost["wake"]
        order.append(item)
        if mark == "Y":
            summing.append(item[1:])

    def serve():
        busy = False
        for tag in [t for t in summing if landed[("Y", *t)] <= clock]:
            summing.remove(tag)
            run(("F", *tag))
            start(("X", *tag))
            start(("E", *tag))
            passing.append(tag)
            placing.append((("R", *tag), ("E", *tag)))
            busy = True
        for tag in [t for t in passing if landed[("X", *t)] <= clock]:
            passing.remove(tag)
            start(("G", *tag))
            placing.extend([(("Q", *tag), ("X", *tag)), (("T", *tag), ("G", *tag))])
            busy = True
        return busy

    def put():
        for entry in placing:
            if landed[entry[1]] <= clock:
                placing.remove(entry)
                run(entry[0])
                return True
        return False

    for item in plan:
        if item[0] in SENDS:
            start(item)
            continue
        serve()
        while free["Y"] - clock > cost["ahead"] and put():
            serve()
        run(item)
    while summing or passing or placing:
        if not (serve() or put()):
            times = [landed[("Y", *t)] for t in summing] + [landed[("X", *t)] for t in passing] + [landed[e[1]] for e in placing]
            clock = max(clock, min(times))
    return order


def gelu_fn(value):
    return jax.nn.gelu(value, approximate=True)


def gelu_slope(value):
    square = value * value
    t = jnp.tanh(value * (ROOT + (ROOT * CUBIC) * square))
    return (0.5 + 0.5 * t) + (value * (0.5 * ROOT + (1.5 * ROOT * CUBIC) * square)) * (1.0 - t * t)


def dot(left, right, dims):
    return lax.dot_general(left, right, dims, preferred_element_type=F32)


def blank(shape):
    return pl.pallas_call(
        lambda out: None,
        out_shape=jax.ShapeDtypeStruct(shape, F32),
        out_specs=pl.BlockSpec(memory_space=pl.ANY),
    )()


PARAMS = pltpu.CompilerParams(vmem_limit_bytes=67_043_328)


def work(rows, depth, columns, moved):
    return pl.CostEstimate(flops=2 * rows * depth * columns, bytes_accessed=moved, transcendentals=0)


def up_kernel(layer, hidden, w_in):
    rows, width = hidden.shape
    ff = w_in.shape[2]
    tile, chunk = 512, 128

    def body(h_ref, w_ref, u_ref, a_ref):
        last = None
        for first in [*range(0, rows, chunk), None]:
            if first is not None:
                part = pl.ds(first, chunk)
                u_ref[part, :] = dot(h_ref[part, :], w_ref[0], NN).astype(BF16)
            if last is not None:
                part = pl.ds(last, chunk)
                a_ref[part, :] = gelu_fn(u_ref[part, :].astype(F32)).astype(BF16)
            last = first

    return pl.pallas_call(
        body,
        grid=(ff // tile,),
        in_specs=[pl.BlockSpec((rows, width), lambda j: (0, 0)), pl.BlockSpec((1, width, tile), lambda j: (layer, 0, j))],
        out_specs=[pl.BlockSpec((rows, tile), lambda j: (0, j))] * 2,
        out_shape=[jax.ShapeDtypeStruct((rows, ff), BF16)] * 2,
        compiler_params=PARAMS,
        cost_estimate=work(rows, width, ff, 60_000_000),
    )(hidden, w_in)


def back_kernel(layer, cot, w_out, pre):
    rows, width = cot.shape
    ff = pre.shape[1]
    tile, chunk = 512, 256

    def body(g_ref, w_ref, u_ref, v_ref):
        for first in range(0, rows, chunk):
            part = pl.ds(first, chunk)
            v_ref[part, :] = (dot(g_ref[part, :], w_ref[0], NT) * gelu_slope(u_ref[part, :].astype(F32))).astype(BF16)

    return pl.pallas_call(
        body,
        grid=(ff // tile,),
        in_specs=[
            pl.BlockSpec((rows, width), lambda j: (0, 0)),
            pl.BlockSpec((1, tile, width), lambda j: (layer, j, 0)),
            pl.BlockSpec((rows, tile), lambda j: (0, j)),
        ],
        out_specs=pl.BlockSpec((rows, tile), lambda j: (0, j)),
        out_shape=jax.ShapeDtypeStruct((rows, ff), BF16),
        compiler_params=PARAMS,
        cost_estimate=work(rows, width, ff, 60_000_000),
    )(cot, w_out, pre)


def forward_kernel(layer, hidden, w_in, w_out, target=None, scale=1.0):
    rows, width = hidden.shape
    ff = w_in.shape[2]
    tile, chunk = 512, 128
    steps = ff // tile

    def body(h_ref, up_ref, down_ref, *rest):
        u_ref, a_ref, next_ref, total = rest[-4:]
        step = pl.program_id(0)

        @pl.when(step == 0)
        def _():
            total[...] = h_ref[...].astype(F32)

        firsts = list(range(0, rows, chunk))
        for index in range(len(firsts) + 2):
            if index < len(firsts):
                part = pl.ds(firsts[index], chunk)
                u_ref[part, :] = dot(h_ref[part, :], up_ref[0], NN).astype(BF16)
            if 1 <= index <= len(firsts):
                part = pl.ds(firsts[index - 1], chunk)
                a_ref[part, :] = gelu_fn(u_ref[part, :].astype(F32)).astype(BF16)
            if index >= 2:
                part = pl.ds(firsts[index - 2], chunk)
                total[part, :] += dot(a_ref[part, :], down_ref[0], NN)

        @pl.when(step == steps - 1)
        def _():
            result = total[...].astype(BF16)
            if target is not None:
                result = ((result.astype(F32) - rest[0][...].astype(F32)) * scale).astype(BF16)
            next_ref[...] = result

    whole = pl.BlockSpec((rows, width), lambda j: (0, 0))
    column = pl.BlockSpec((rows, tile), lambda j: (0, j))
    extra = [] if target is None else [target]
    return pl.pallas_call(
        body,
        grid=(steps,),
        in_specs=[
            whole,
            pl.BlockSpec((1, width, tile), lambda j: (layer, 0, j)),
            pl.BlockSpec((1, tile, width), lambda j: (layer, j, 0)),
        ] + [whole] * len(extra),
        out_specs=[column, column, whole],
        out_shape=[jax.ShapeDtypeStruct((rows, ff), BF16)] * 2 + [jax.ShapeDtypeStruct((rows, width), BF16)],
        scratch_shapes=[pltpu.VMEM((rows, width), F32)],
        compiler_params=PARAMS,
        cost_estimate=work(rows, width, 2 * ff, 80_000_000),
    )(hidden, w_in, w_out, *extra)


def backward_kernel(layer, cot, w_in, w_out, pre):
    rows, width = cot.shape
    ff = pre.shape[1]
    tile, chunk = 512, 256
    steps = ff // tile

    def body(g_ref, down_ref, up_ref, u_ref, v_ref, next_ref, total):
        step = pl.program_id(0)

        @pl.when(step == 0)
        def _():
            total[...] = g_ref[...].astype(F32)

        last = None
        for first in [*range(0, rows, chunk), None]:
            if first is not None:
                part = pl.ds(first, chunk)
                v_ref[part, :] = (dot(g_ref[part, :], down_ref[0], NT) * gelu_slope(u_ref[part, :].astype(F32))).astype(BF16)
            if last is not None:
                part = pl.ds(last, chunk)
                total[part, :] += dot(v_ref[part, :], up_ref[0], NT)
            last = first

        @pl.when(step == steps - 1)
        def _():
            next_ref[...] = total[...].astype(BF16)

    whole = pl.BlockSpec((rows, width), lambda j: (0, 0))
    column = pl.BlockSpec((rows, tile), lambda j: (0, j))
    return pl.pallas_call(
        body,
        grid=(steps,),
        in_specs=[
            whole,
            pl.BlockSpec((1, tile, width), lambda j: (layer, j, 0)),
            pl.BlockSpec((1, width, tile), lambda j: (layer, 0, j)),
            column,
        ],
        out_specs=[column, whole],
        out_shape=[jax.ShapeDtypeStruct((rows, ff), BF16), jax.ShapeDtypeStruct((rows, width), BF16)],
        scratch_shapes=[pltpu.VMEM((rows, width), F32)],
        compiler_params=PARAMS,
        cost_estimate=work(rows, width, 2 * ff, 80_000_000),
    )(cot, w_out, w_in, pre)


def gradient_kernel(which, sliced, left, right, theirs, pieces):
    rows = left[0].shape[0]
    blk = 1280
    tile, chunk = 512, 128
    height = blk // pieces
    ends = (256, 640, 896, blk)
    cuts = sorted({0, *ends, *range(0, blk, height)})
    ranges = [(first, last - first) for first, last in zip(cuts, cuts[1:])]
    half = rows // tile
    steps = 2 * half

    def spec(name, far):
        def index(k, which):
            row = jnp.maximum(k - half, 0) if far else jnp.minimum(k, half - 1)
            return row, (which[0] if name == sliced else 0)

        return pl.BlockSpec((tile, blk), index)

    def body(which_ref, lo, lf, ro, rf, *rest):
        theirs_ref = rest[0] if theirs is not None else None
        outs = rest[1 if theirs is not None else 0:][:pieces]
        total, out_sems = rest[-2 - (2 if theirs is not None else 0):][:2]
        step = pl.program_id(0)

        def product(l_ref, r_ref, first):
            return dot(l_ref[:, pl.ds(first, chunk)], r_ref[...], TN)

        if theirs is not None:
            other, other_sem = rest[-2:]
            fetch = pltpu.make_async_copy(theirs_ref, other, other_sem)

        @pl.when(step == 0)
        def _():
            if theirs is not None:
                fetch.start()
            for first in range(0, blk, chunk):
                total[pl.ds(first, chunk), :] = product(lo, ro, first)

        @pl.when(jnp.logical_and(step > 0, step < half))
        def _():
            for first in range(0, blk, chunk):
                total[pl.ds(first, chunk), :] += product(lo, ro, first)

        @pl.when(jnp.logical_and(step >= half, step < steps - 1))
        def _():
            for first in range(0, blk, chunk):
                total[pl.ds(first, chunk), :] += product(lf, rf, first)

        @pl.when(step == steps - 1)
        def _():
            if theirs is not None:
                fetch.wait()
            copies = []
            for first in range(0, blk, chunk):
                part = pl.ds(first, chunk)
                value = total[part, :] + product(lf, rf, first)
                total[part, :] = value if theirs is None else value + other[part, :]
                if first + chunk in ends:
                    for start, count in ranges[len(copies):]:
                        if start + count > first + chunk:
                            break
                        piece, offset = divmod(start, height)
                        copies.append(pltpu.make_async_copy(
                            total.at[pl.ds(start, count), :], outs[piece].at[pl.ds(offset, count), :], out_sems.at[len(copies)]))
                        copies[-1].start()
            for copy in copies:
                copy.wait()

    anywhere = pl.BlockSpec(memory_space=pl.ANY)
    extra = [] if theirs is None else [theirs]
    scratch = [pltpu.VMEM((blk, blk), F32), pltpu.SemaphoreType.DMA((len(ranges),))]
    if theirs is not None:
        scratch += [pltpu.VMEM((blk, blk), F32), pltpu.SemaphoreType.DMA(())]
    return pl.pallas_call(
        body,
        grid_spec=pltpu.PrefetchScalarGridSpec(
            num_scalar_prefetch=1,
            grid=(steps,),
            in_specs=[spec("left", False), spec("left", True), spec("right", False), spec("right", True)] + [anywhere] * len(extra),
            out_specs=[anywhere] * pieces,
            scratch_shapes=scratch,
        ),
        out_shape=[jax.ShapeDtypeStruct((blk // pieces, blk), F32)] * pieces,
        compiler_params=PARAMS,
        cost_estimate=work(2 * rows, blk, blk, 40_000_000),
    )(which, *left, *right, *extra)


def solution(mesh):
    order = issue_order(PIECES, COST)
    group = mesh.shape["data"]
    to_core = [(i, i ^ 1) for i in range(group)]
    to_x = [(i, i ^ 2) for i in range(group)]
    to_y = [(i, i ^ 4) for i in range(group)]
    route = {"X": to_x, "Y": to_y, "D": to_core, "E": to_core, "G": to_core}

    def local_step(tokens, targets, w_in, w_out):
        rows = tokens.shape[0]
        layers, width, ff = w_in.shape
        blk = ff // 4
        scale = 1.0 / math.sqrt(rows * group)
        me = lax.axis_index("data") & 3
        starts = [pl.multiple_of((me ^ flip) * blk, blk) for flip in range(4)]
        blocks = [jnp.reshape(me ^ flip, (1,)).astype(jnp.int32) for flip in range(2)]
        grads = {"A": blank((layers, ff, width)), "B": blank((layers, width, ff))}
        val = {("o", "h0"): tokens}

        def forward(side, layer):
            last = layer == layers - 1
            pre, act, after = forward_kernel(layer, val[side, f"h{layer}"], w_in, w_out, targets if last else None, scale)
            val[side, f"u{layer}"], val[side, f"a{layer}"] = pre, act
            val[side, f"g{layers}" if last else f"h{layer + 1}"] = after

        def up(side, layer):
            val[side, f"u{layer}"], val[side, f"a{layer}"] = up_kernel(layer, val[side, f"h{layer}"], w_in)

        def backward(side, layer):
            val[side, f"v{layer}"], val[side, f"g{layer}"] = backward_kernel(
                layer, val[side, f"g{layer + 1}"], w_in, w_out, val[side, f"u{layer}"])

        def back_act(side, layer):
            val[side, f"v{layer}"] = back_kernel(layer, val[side, f"g{layer + 1}"], w_out, val[side, f"u{layer}"])

        def partial_sum(name, block):
            kind, layer = name[0], int(name[1])
            left, right = ("a", f"g{layer + 1}") if kind == "A" else ("h", f"v{layer}")
            left = [val[side, f"{left}{layer}"] for side in "of"]
            right = [val[side, right] for side in "of"]
            mine = block == "m"
            parts = gradient_kernel(
                blocks[0 if mine else 1], "left" if kind == "A" else "right", left, right,
                val["D", name] if mine else None, PIECES[name] if mine else 1)
            if mine:
                for piece, part in enumerate(parts):
                    val[name, piece] = part
            else:
                val[name, "s"] = parts[0]

        def place(mark, name, piece):
            if mark == "F":
                val["F", name, piece] = val[name, piece] + val["Y", name, piece]
            source, which = PLACES[mark]
            block, start = val[source, name, piece], starts[which]
            kind, layer = name[0], int(name[1])
            first = piece * block.shape[0]
            where = (layer, start + first, 0) if kind == "A" else (layer, first, start)
            grads[kind] = lax.dynamic_update_slice(grads[kind], block[None], where)

        def operation(item):
            mark = item[0]
            if mark in PIECES:
                partial_sum(*item)
            elif mark in PLACES:
                place(*item)
            else:
                {"w": forward, "u": up, "b": backward, "v": back_act}[item[1]](mark, item[2])

        def transfer(item):
            mark, rest = item[0], item[1:]
            if rest[0] not in PIECES:
                val["f", rest[0]] = lax.ppermute(val["o", rest[0]], "data", to_x)
                return
            source = {"X": ("F", *rest), "E": ("F", *rest), "G": ("X", *rest), "Y": rest, "D": (rest[0], "s")}[mark]
            val[item] = lax.ppermute(val[source], "data", route[mark])

        for item in order:
            (transfer if item[0] in SENDS else operation)(item)
        return grads["B"], grads["A"]

    return jax.shard_map(local_step, mesh=mesh, in_specs=(P("data"), P("data"), P(), P()), out_specs=(P(), P()), check_vma=False)
```
